32 devices in a mesh: dp: 16 (over z, y, x), layer: 2 (over core).
Axes of the slice: x: 2, y: 2, z: 4, core: 2. Of those that a mesh axis runs over, the one named last changes fastest.
Arguments:
- layer_inputs: bfloat16 [2, 16384, 4096], P('layer', 'dp'), may hold values from -6 to 6
- output_grads: bfloat16 [2, 16384, 512], P('layer', 'dp'), may hold values from -6 to 6
- input_factors: bfloat16 [128, 2, 4, 4096], P('dp', 'layer'), may hold values from -0.09375 to 0.09375
- output_factors: bfloat16 [128, 2, 4, 512], P('dp', 'layer'), may hold values from -0.25 to 0.25
Outputs:
- scores: float32 [128, 16384], P(None, 'dp')
The draws below stay inside these ranges and needn't reach their ends.
All inputs are finite; a program needn't handle non-finite values.
Results may differ from the reference program's by a relative error of at most 0.0003.
Values may be sent and summed in bfloat16 or wider, within the bound.
A program may use at most 128 MiB of HBM per device.

```python
import jax
import jax.numpy as jnp
from jax import lax

D = 4096
KV = 512
RANK = 4
LAYERS = 2
TOKENS = 16384
QUERIES = 128


def shard_levels(key, extent, shards, least, high):
    gain = 1.0
    for dim, blocks in shards:
        steps = jax.random.uniform(jax.random.fold_in(jax.random.fold_in(key, 6), dim), (blocks,), jnp.float32, least / len(shards), high / len(shards))
        gain = gain * jnp.repeat(jnp.exp(steps), extent[dim] // blocks).reshape((-1,) + (1,) * (len(extent) - 1 - dim))
    return gain


def gaussian(rng, dims, deviation, most, shards=(), held_as=jnp.bfloat16):
    entries = jax.random.normal(rng, dims, jnp.float32) * deviation
    if len(shards) > 0:
        entries = shard_levels(rng, dims, shards, -0.22, 0.18) * entries
    return jnp.clip(entries, min=-most, max=most).astype(held_as)


def setup_inputs(seed: int = 0) -> dict:
    key_of = jax.random.split(jax.random.key(seed), 5)
    return {
        "layer_inputs": gaussian(key_of[0], (LAYERS, TOKENS, D), 1.0, 6.0, ((0, 2), (1, 16))),
        "output_grads": gaussian(key_of[1], (LAYERS, TOKENS, KV), 1.0, 6.0, ((0, 2), (1, 16))),
        "input_factors": gaussian(key_of[2], (QUERIES, LAYERS, RANK, D), D ** -0.5, 0.09375, ((0, 16), (1, 2))),
        "output_factors": gaussian(key_of[3], (QUERIES, LAYERS, RANK, KV), KV ** -0.5, 0.25, ((0, 16), (1, 2))),
    }


def layer_term(acts, grads, in_fac, out_fac):
    count = in_fac.shape[0]
    in_flat = in_fac.reshape(count * in_fac.shape[1], in_fac.shape[2])
    out_flat = out_fac.reshape(count * out_fac.shape[1], out_fac.shape[2])
    proj_in = lax.dot_general(acts, in_flat, (((1,), (1,)), ((), ())), preferred_element_type=jnp.float32)
    proj_out = lax.dot_general(grads, out_flat, (((1,), (1,)), ((), ())), preferred_element_type=jnp.float32)
    joined = (proj_in * proj_out).reshape(acts.shape[0], count, in_fac.shape[1])
    return jnp.sum(joined, axis=2).T


def reference(layer_inputs, output_grads, input_factors, output_factors):
    in_layers = jnp.moveaxis(input_factors, 1, 0)
    out_layers = jnp.moveaxis(output_factors, 1, 0)

    def step(total, items):
        acts, grads, in_fac, out_fac = items
        return total + layer_term(acts, grads, in_fac, out_fac), None

    start = jnp.zeros((QUERIES, TOKENS), jnp.float32)
    total, unused = lax.scan(step, start, (layer_inputs, output_grads, in_layers, out_layers))
    return total
```

```python
import functools

import jax
import jax.numpy as jnp
from jax import lax
from jax.experimental import pallas as pl
from jax.experimental.pallas import tpu as pltpu
from jax.sharding import PartitionSpec as P

MESH = pl.DeviceIdType.MESH
OWN, ACROSS_X, ACROSS_Y, DIAG = range(4)
LINKS = ("x", "y", "in", "ex")
CUTS = 4
BATCH = 4
AHEAD = 2
LATENCY = 1.6
RATE = 730.0
COMPUTE = 0.8
TUNED = {
    4: {
        (0, "x"): ((ACROSS_Y, 0), (OWN, 2), (OWN, 0), (ACROSS_Y, 2), (OWN, 1), (OWN, 3)),
        (0, "in"): ((OWN, 0), (DIAG, 2), (DIAG, 0)),
        (1, "x"): ((ACROSS_Y, 1), (OWN, 3), (OWN, 1), (OWN, 0), (ACROSS_Y, 3), (OWN, 2)),
        (1, "in"): ((OWN, 1), (OWN, 0)),
        (1, "ex"): ((OWN, 2), (OWN, 3), (DIAG, 1), (OWN, 1), (DIAG, 3)),
    }
}


def rank_of(nz, end, link, kind, level, piece):
    if link == "y":
        link, kind = "x", {ACROSS_X: ACROSS_Y}.get(kind, kind)
    if nz in TUNED:
        return TUNED[nz][end, link].index((kind, level)), piece
    away = abs(level - end)
    if link == "x":
        return away + (0.5 if kind != OWN else 0.0), piece
    return away + (1.5 if kind != OWN else 0.0), piece


def receiver(half, nz, end, link, level):
    if link in ("x", "y"):
        return end, level
    if link == "ex":
        return end - 1, level
    return (end + 1, level) if end + 1 < half else (end, nz - 1 - level)


def simulate(nz, widths):
    half, pieces = nz // 2, range(len(widths))
    todo, avail = {}, {}
    for end in range(half):
        queue = {link: [] for link in LINKS}
        for level in range(nz):
            for piece in pieces:
                queue["x"].append((OWN, level, piece, ACROSS_X))
                queue["y"].append((OWN, level, piece, ACROSS_Y))
                if level % 2 == end % 2:
                    if (level // 2 + piece) % 2 == 0:
                        queue["x"].append((ACROSS_Y, level, piece, DIAG))
                    else:
                        queue["y"].append((ACROSS_X, level, piece, DIAG))
                    queue["in" if end % 2 == 0 else "ex"].append((DIAG, level, piece, DIAG))
                if level <= end:
                    queue["in"].append((OWN, level, piece, OWN))
                if level >= end > 0:
                    queue["ex"].append((OWN, level, piece, OWN))
        for piece in pieces:
            avail[end, OWN, end, piece] = 0.0
        todo.update({(end, link): items for link, items in queue.items() if items})
    free = {key: 0.0 for key in todo}
    sent = {key: [] for key in todo}
    while any(todo.values()):
        best = None
        for key, items in todo.items():
            for item in items:
                start = max(free[key], avail.get((key[0], *item[:3]), 1e9))
                if best is None or start < best[0] - 1e-9:
                    best = (start, key, [])
                if best[1] == key and start <= best[0] + 1e-9:
                    best[2].append(item)
        start, (end, link), ready = best
        item = min(ready, key=lambda it: rank_of(nz, end, link, *it[:3]))
        todo[end, link].remove(item)
        free[end, link] = start + widths[item[2]] / RATE
        there, level = receiver(half, nz, end, link, item[1])
        avail[there, item[3], level, item[2]] = free[end, link] + LATENCY
        sent[end, link].append((start, item))
    return sent, avail


def plan(nz, widths):
    half, pieces = nz // 2, len(widths)
    sent, avail = simulate(nz, widths)
    slot = {}
    for end in range(half):
        shares = [(kind, level) for kind in range(4) for level in range(nz)]
        shares.sort(key=lambda s: (s != (OWN, end), max(avail[end, *s, p] for p in range(pieces))))
        slot[end] = {share: at for at, share in enumerate(shares)}
    steps = [(batch, piece) for batch in range(4 * nz // BATCH) for piece in range(pieces)]
    events = {}
    for end in range(half):
        found = []
        for (sender, link), items in sent.items():
            if sender != end:
                continue
            for i, (start, (kind, level, piece, arrives)) in enumerate(items):
                at = max(avail[end, kind, level, piece], items[i - AHEAD][0] if i >= AHEAD else 0.0)
                there, counted = receiver(half, nz, end, link, level)
                found.append((at, 0, len(found), ("send", link, i, slot[end][kind, level], slot[there][arrives, counted], piece)))
        order = sorted(found)
        events[end], clock, done = [], 0.0, 0
        members = {}
        for share, at in slot[end].items():
            members.setdefault(at // BATCH, []).append((share, at))
        for batch, piece in steps:
            need = [(avail[end, *share, piece], at) for share, at in members[batch]]
            clock = max([clock] + [t for t, _ in need])
            part = []
            while done < len(order) and order[done][0] <= clock:
                part.append(order[done])
                done += 1
            part += [(t, 1, at, ("wait", at, piece)) for t, at in need]
            events[end].append([event for *_, event in sorted(part)])
            clock += COMPUTE * widths[piece] / 1024
        events[end].append([event for *_, event in order[done:]])
    return slot, steps, events


def kernel(nz, layers, count, rank, widths, in_hbm, ofac_hbm, acts_hbm, grads_hbm, out_ref,
           raw_in, raw_out, slots_in, slots_out, acts, grads, total, parts,
           load_sem, recv_sem, send_sem, psend_sem, precv_sem):
    me = lax.axis_index("dp")
    layer = lax.axis_index("layer")
    x, y, z = me % 2, (me // 2) % 2, me // 4
    half = nz // 2
    rows = count * rank
    tokens = acts.shape[0]
    cut = slots_in.shape[2]
    low = z < half
    end = jnp.where(low, z, nz - 1 - z)
    inward = jnp.where(low, 4, 4 * nz - 4)
    target = {
        "x": {"dp": me + 1 - 2 * x},
        "y": {"dp": me + 2 - 4 * y},
        "in": {"dp": (me + inward) % (4 * nz)},
        "ex": {"dp": (me + 4 * nz - inward) % (4 * nz)},
    }
    slot, steps, events = plan(nz, widths)

    load_in = pltpu.make_async_copy(in_hbm, raw_in, load_sem.at[0])
    load_out = pltpu.make_async_copy(ofac_hbm, raw_out, load_sem.at[1])
    load_acts = pltpu.make_async_copy(acts_hbm, acts, load_sem.at[2])
    load_grads = pltpu.make_async_copy(grads_hbm, grads, load_sem.at[3])
    load_in.start()
    load_out.start()
    load_acts.start()
    load_grads.start()

    barrier = pltpu.get_barrier_semaphore()
    for link in ("x", "y", "in"):
        pl.semaphore_signal(barrier, inc=1, device_id=target[link], device_id_type=MESH)
    for k in range(1, layers):
        pl.semaphore_signal(barrier, inc=1, device_id={"layer": (layer + k) % layers}, device_id_type=MESH)

    @pl.when(end > 0)
    def _():
        pl.semaphore_signal(barrier, inc=1, device_id=target["ex"], device_id_type=MESH)

    load_in.wait()
    load_out.wait()
    for piece in range(len(widths) - 1):
        own = jnp.swapaxes(raw_in[:, :, piece * cut:(piece + 1) * cut], 0, 1).reshape(rows, cut)
        slots_in[piece, :rows, :] = own
    slots_out[:rows, :] = jnp.swapaxes(raw_out[...], 0, 1).reshape(rows, slots_out.shape[1])
    pl.semaphore_wait(barrier, 3 + layers - 1 + jnp.where(end > 0, 1, 0))

    def held(at, piece):
        span = pl.ds(at * rows, rows)
        return slots_in.at[piece, span, :] if piece < len(widths) - 1 else slots_out.at[span, :]

    def send(link, i, source, dest, piece):
        return pltpu.make_async_remote_copy(
            src_ref=held(source, piece),
            dst_ref=held(dest, piece),
            send_sem=send_sem.at[LINKS.index(link), i],
            recv_sem=recv_sem.at[dest, piece],
            device_id=target[link],
            device_id_type=MESH,
        )

    def arrived(at, piece):
        pltpu.make_async_remote_copy(
            src_ref=held(at, piece),
            dst_ref=held(at, piece),
            send_sem=send_sem.at[0, 0],
            recv_sem=recv_sem.at[at, piece],
            device_id=target["x"],
            device_id_type=MESH,
        ).wait_recv()

    seen = {k: {(0, piece) for piece in range(len(widths))} for k in range(half)}

    def communicate(step):
        for k in range(half):
            def act(k=k):
                for what, *args in events[k][step]:
                    source, piece = (args[2], args[4]) if what == "send" else args
                    if (source, piece) not in seen[k]:
                        seen[k].add((source, piece))
                        arrived(source, piece)
                    if what == "send":
                        send(*args).start()

            if events[k][step]:
                pl.when(end == k)(act)

    chunk = min(256, tokens)
    group = BATCH * rows
    dims = (((1,), (1,)), ((), ()))

    def multiply(batch, piece):
        def body(i, carry):
            cols = pl.ds(pl.multiple_of(i * chunk, chunk), chunk)
            span = slice(batch * group, (batch + 1) * group)
            if piece < len(widths) - 1:
                left, right = slots_in[piece, span, :], acts[cols, piece * cut:(piece + 1) * cut]
                term = lax.dot_general(left, right, dims, preferred_element_type=jnp.float32)
                total[:, cols] = term if piece == 0 else total[:, cols] + term
            else:
                proj_out = lax.dot_general(slots_out[span, :], grads[cols, :], dims, preferred_element_type=jnp.float32)
                joined = (total[:, cols] * proj_out).reshape(BATCH, rank, count, chunk)
                parts[layer, batch, :, cols] = jnp.sum(joined, axis=1).reshape(BATCH * count, chunk)
            return carry

        lax.fori_loop(0, tokens // chunk, body, 0)

    def share(batch, k, to):
        return pltpu.make_async_remote_copy(
            src_ref=parts.at[to, batch],
            dst_ref=parts.at[to, batch],
            send_sem=psend_sem.at[batch, k],
            recv_sem=precv_sem.at[batch, to],
            device_id={"layer": (layer + k) % layers},
            device_id_type=MESH,
        )

    def finish(batch):
        for k in range(1, layers):
            share(batch, k, (layer + k) % layers).wait_recv()
        for i in range(BATCH):
            base = 0
            for k in range(half):
                kind, level = [share for share, at in slot[k].items() if at == batch * BATCH + i][0]
                col = ((1 - y) if kind in (ACROSS_Y, DIAG) else y) * 2 + ((1 - x) if kind in (ACROSS_X, DIAG) else x)
                at = jnp.where(low, level, nz - 1 - level) * 4 + col
                base = base + jnp.where(end == k, at, 0)
            score = parts[0, batch, i * count:(i + 1) * count, :]
            for other in range(1, layers):
                score = score + parts[other, batch, i * count:(i + 1) * count, :]
            out_ref[pl.ds(pl.multiple_of(base * count, count), count), :] = score

    for step, (batch, piece) in enumerate(steps):
        communicate(step)
        if step == 0:
            load_acts.wait()
            load_grads.wait()
        multiply(batch, piece)
        if piece == 0 and batch > 0:
            finish(batch - 1)
        if piece == len(widths) - 1:
            for k in range(1, layers):
                share(batch, k, layer).start()
    communicate(len(steps))
    finish(steps[-1][0])

    for k in range(half):
        def sent(k=k):
            for what, *args in sum(events[k], []):
                if what == "send":
                    send(*args).wait_send()

        pl.when(end == k)(sent)
    for batch in range(steps[-1][0] + 1):
        for k in range(1, layers):
            share(batch, k, layer).wait_send()


def shards(nz, layers, layer_inputs, output_grads, input_factors, output_factors):
    count, _, rank, d_in = input_factors.shape
    d_out = output_factors.shape[3]
    tokens = layer_inputs.shape[1]
    rows, cut = count * rank, d_in // CUTS
    widths = (cut,) * CUTS + (d_out,)
    slots = 4 * nz
    queue = max(len(items) for items in simulate(nz, widths)[0].values())
    dma = pltpu.SemaphoreType.DMA
    return pl.pallas_call(
        functools.partial(kernel, nz, layers, count, rank, widths),
        out_shape=jax.ShapeDtypeStruct((slots * count, tokens), jnp.float32),
        in_specs=[pl.BlockSpec(memory_space=pl.ANY)] * 4,
        out_specs=pl.BlockSpec(memory_space=pltpu.VMEM),
        scratch_shapes=[
            pltpu.VMEM((count, rank, d_in), jnp.bfloat16),
            pltpu.VMEM((count, rank, d_out), jnp.bfloat16),
            pltpu.VMEM((CUTS, slots * rows, cut), jnp.bfloat16),
            pltpu.VMEM((slots * rows, d_out), jnp.bfloat16),
            pltpu.VMEM((tokens, d_in), jnp.bfloat16),
            pltpu.VMEM((tokens, d_out), jnp.bfloat16),
            pltpu.VMEM((BATCH * rows, tokens), jnp.float32),
            pltpu.VMEM((layers, slots // BATCH, BATCH * count, tokens), jnp.float32),
            dma((4,)),
            dma((slots, CUTS + 1)),
            dma((4, queue)),
            dma((slots // BATCH, layers)),
            dma((slots // BATCH, layers)),
        ],
        compiler_params=pltpu.CompilerParams(
            collective_id=0, has_side_effects=True, vmem_limit_bytes=60 * 1024 * 1024
        ),
    )(input_factors[:, 0], output_factors[:, 0], layer_inputs[0], output_grads[0])


def solution(mesh):
    in_specs = (
        P("layer", "dp", None),
        P("layer", "dp", None),
        P("dp", "layer", None, None),
        P("dp", "layer", None, None),
    )
    body = functools.partial(shards, mesh.shape["dp"] // 4, mesh.shape["layer"])
    return jax.shard_map(body, mesh=mesh, in_specs=in_specs, out_specs=P(None, "dp"), check_vma=False)
```

```python
import functools

import jax
import jax.numpy as jnp
from jax import lax
from jax.experimental import pallas as pl
from jax.experimental.pallas import tpu as pltpu
from jax.sharding import PartitionSpec as P

MESH = pl.DeviceIdType.MESH
OWN, ACROSS_X, ACROSS_Y, DIAG = range(4)
LINKS = ("x", "y", "in", "ex")
CUTS = 2
BATCH = 4
AHEAD = 2
LATENCY = 1.6
RATE = 730.0
COMPUTE = 0.8
TUNED = {
    4: {
        (0, "x"): ((ACROSS_Y, 0), (OWN, 2), (OWN, 0), (ACROSS_Y, 2), (OWN, 1), (OWN, 3)),
        (0, "in"): ((OWN, 0), (DIAG, 2), (DIAG, 0)),
        (1, "x"): ((ACROSS_Y, 1), (OWN, 3), (OWN, 1), (OWN, 0), (ACROSS_Y, 3), (OWN, 2)),
        (1, "in"): ((OWN, 1), (OWN, 0)),
        (1, "ex"): ((OWN, 2), (OWN, 3), (DIAG, 1), (OWN, 1), (DIAG, 3)),
    }
}


def rank_of(nz, end, link, kind, level, piece):
    if link == "y":
        link, kind = "x", {ACROSS_X: ACROSS_Y}.get(kind, kind)
    if nz in TUNED:
        return TUNED[nz][end, link].index((kind, level)), piece
    away = abs(level - end)
    if link == "x":
        return away + (0.5 if kind != OWN else 0.0), piece
    return away + (1.5 if kind != OWN else 0.0), piece


def receiver(half, nz, end, link, level):
    if link in ("x", "y"):
        return end, level
    if link == "ex":
        return end - 1, level
    return (end + 1, level) if end + 1 < half else (end, nz - 1 - level)


def simulate(nz, widths):
    half, pieces = nz // 2, range(len(widths))
    todo, avail = {}, {}
    for end in range(half):
        queue = {link: [] for link in LINKS}
        for level in range(nz):
            for piece in pieces:
                queue["x"].append((OWN, level, piece, ACROSS_X))
                queue["y"].append((OWN, level, piece, ACROSS_Y))
                if level % 2 == end % 2:
                    if (level // 2 + piece) % 2 == 0:
                        queue["x"].append((ACROSS_Y, level, piece, DIAG))
                    else:
                        queue["y"].append((ACROSS_X, level, piece, DIAG))
                    queue["in" if end % 2 == 0 else "ex"].append((DIAG, level, piece, DIAG))
                if level <= end:
                    queue["in"].append((OWN, level, piece, OWN))
                if level >= end > 0:
                    queue["ex"].append((OWN, level, piece, OWN))
        for piece in pieces:
            avail[end, OWN, end, piece] = 0.0
        todo.update({(end, link): items for link, items in queue.items() if items})
    free = {key: 0.0 for key in todo}
    sent = {key: [] for key in todo}
    while any(todo.values()):
        best = None
        for key, items in todo.items():
            for item in items:
                start = max(free[key], avail.get((key[0], *item[:3]), 1e9))
                if best is None or start < best[0] - 1e-9:
                    best = (start, key, [])
                if best[1] == key and start <= best[0] + 1e-9:
                    best[2].append(item)
        start, (end, link), ready = best
        item = min(ready, key=lambda it: rank_of(nz, end, link, *it[:3]))
        todo[end, link].remove(item)
        free[end, link] = start + widths[item[2]] / RATE
        there, level = receiver(half, nz, end, link, item[1])
        avail[there, item[3], level, item[2]] = free[end, link] + LATENCY
        sent[end, link].append((start, item))
    return sent, avail


def plan(nz, widths):
    half, pieces = nz // 2, len(widths)
    sent, avail = simulate(nz, widths)
    slot = {}
    for end in range(half):
        shares = [(kind, level) for kind in range(4) for level in range(nz)]
        shares.sort(key=lambda s: (s != (OWN, end), max(avail[end, *s, p] for p in range(pieces))))
        slot[end] = {share: at for at, share in enumerate(shares)}
    steps = [(batch, piece) for batch in range(4 * nz // BATCH) for piece in range(pieces)]
    events = {}
    for end in range(half):
        found = []
        for (sender, link), items in sent.items():
            if sender != end:
                continue
            at = 0.0
            for i, (start, (kind, level, piece, arrives)) in enumerate(items):
                at = max(at, avail[end, kind, level, piece], items[i - AHEAD][0] if i >= AHEAD else 0.0)
                there, counted = receiver(half, nz, end, link, level)
                found.append((at, 0, len(found), ("send", link, i, slot[end][kind, level], slot[there][arrives, counted], piece)))
        order = sorted(found)
        events[end], clock, done = [], 0.0, 0
        members = {}
        for share, at in slot[end].items():
            members.setdefault(at // BATCH, []).append((share, at))
        for batch, piece in steps:
            need = [(avail[end, *share, piece], at) for share, at in members[batch]]
            clock = max([clock] + [t for t, _ in need])
            part = []
            while done < len(order) and order[done][0] <= clock:
                part.append(order[done])
                done += 1
            part += [(t, 1, at, ("wait", at, piece)) for t, at in need]
            events[end].append([event for *_, event in sorted(part)])
            clock += COMPUTE * widths[piece] / 1024
        events[end].append([event for *_, event in order[done:]])
    return slot, steps, events


def kernel(nz, layers, count, rank, widths, in_hbm, ofac_hbm, acts_hbm, grads_hbm, out_ref,
           raw_in, raw_out, slots_in, slots_out, acts, grads, total, parts,
           load_sem, recv_sem, send_sem, psend_sem, precv_sem):
    me = lax.axis_index("dp")
    layer = lax.axis_index("layer")
    x, y, z = me % 2, (me // 2) % 2, me // 4
    half = nz // 2
    rows = count * rank
    tokens = acts.shape[0]
    cut = slots_in.shape[2]
    low = z < half
    end = jnp.where(low, z, nz - 1 - z)
    inward = jnp.where(low, 4, 4 * nz - 4)
    target = {
        "x": {"dp": me + 1 - 2 * x},
        "y": {"dp": me + 2 - 4 * y},
        "in": {"dp": (me + inward) % (4 * nz)},
        "ex": {"dp": (me + 4 * nz - inward) % (4 * nz)},
    }
    slot, steps, events = plan(nz, widths)

    load_in = pltpu.make_async_copy(in_hbm, raw_in, load_sem.at[0])
    load_out = pltpu.make_async_copy(ofac_hbm, raw_out, load_sem.at[1])
    load_acts = pltpu.make_async_copy(acts_hbm, acts, load_sem.at[2])
    load_grads = pltpu.make_async_copy(grads_hbm, grads, load_sem.at[3])
    load_in.start()
    load_out.start()
    load_acts.start()
    load_grads.start()

    barrier = pltpu.get_barrier_semaphore()
    for link in ("x", "y", "in"):
        pl.semaphore_signal(barrier, inc=1, device_id=target[link], device_id_type=MESH)
    for k in range(1, layers):
        pl.semaphore_signal(barrier, inc=1, device_id={"layer": (layer + k) % layers}, device_id_type=MESH)

    @pl.when(end > 0)
    def _():
        pl.semaphore_signal(barrier, inc=1, device_id=target["ex"], device_id_type=MESH)

    load_in.wait()
    load_out.wait()
    for piece in range(len(widths) - 1):
        own = jnp.swapaxes(raw_in[:, :, piece * cut:(piece + 1) * cut], 0, 1).reshape(rows, cut)
        slots_in[piece, :rows, :] = own
    slots_out[:rows, :] = jnp.swapaxes(raw_out[...], 0, 1).reshape(rows, slots_out.shape[1])
    pl.semaphore_wait(barrier, 3 + layers - 1 + jnp.where(end > 0, 1, 0))

    def held(at, piece):
        span = pl.ds(at * rows, rows)
        return slots_in.at[piece, span, :] if piece < len(widths) - 1 else slots_out.at[span, :]

    def send(link, i, source, dest, piece):
        return pltpu.make_async_remote_copy(
            src_ref=held(source, piece),
            dst_ref=held(dest, piece),
            send_sem=send_sem.at[LINKS.index(link), i],
            recv_sem=recv_sem.at[dest, piece],
            device_id=target[link],
            device_id_type=MESH,
        )

    def arrived(at, piece):
        pltpu.make_async_remote_copy(
            src_ref=held(at, piece),
            dst_ref=held(at, piece),
            send_sem=send_sem.at[0, 0],
            recv_sem=recv_sem.at[at, piece],
            device_id=target["x"],
            device_id_type=MESH,
        ).wait_recv()

    seen = {k: {(0, piece) for piece in range(len(widths))} for k in range(half)}

    def communicate(step):
        for k in range(half):
            def act(k=k):
                for what, *args in events[k][step]:
                    source, piece = (args[2], args[4]) if what == "send" else args
                    if (source, piece) not in seen[k]:
                        seen[k].add((source, piece))
                        arrived(source, piece)
                    if what == "send":
                        send(*args).start()

            if events[k][step]:
                pl.when(end == k)(act)

    chunk = min(1024, tokens)
    group = BATCH * rows
    dims = (((1,), (1,)), ((), ()))

    def multiply(batch, piece):
        def body(i, carry):
            cols = pl.ds(pl.multiple_of(i * chunk, chunk), chunk)
            span = slice(batch * group, (batch + 1) * group)
            if piece < len(widths) - 1:
                left, right = slots_in[piece, span, :], acts[cols, piece * cut:(piece + 1) * cut]
                term = lax.dot_general(left, right, dims, preferred_element_type=jnp.float32)
                total[:, cols] = term if piece == 0 else total[:, cols] + term
            else:
                proj_out = lax.dot_general(slots_out[span, :], grads[cols, :], dims, preferred_element_type=jnp.float32)
                joined = (total[:, cols] * proj_out).reshape(BATCH, rank, count, chunk)
                parts[layer, batch, :, cols] = jnp.sum(joined, axis=1).reshape(BATCH * count, chunk)
            return carry

        lax.fori_loop(0, tokens // chunk, body, 0)

    def share(batch, k, to):
        return pltpu.make_async_remote_copy(
            src_ref=parts.at[to, batch],
            dst_ref=parts.at[to, batch],
            send_sem=psend_sem.at[batch, k],
            recv_sem=precv_sem.at[batch, to],
            device_id={"layer": (layer + k) % layers},
            device_id_type=MESH,
        )

    def finish(batch):
        for k in range(1, layers):
            share(batch, k, (layer + k) % layers).wait_recv()
        for i in range(BATCH):
            base = 0
            for k in range(half):
                kind, level = [share for share, at in slot[k].items() if at == batch * BATCH + i][0]
                col = ((1 - y) if kind in (ACROSS_Y, DIAG) else y) * 2 + ((1 - x) if kind in (ACROSS_X, DIAG) else x)
                at = jnp.where(low, level, nz - 1 - level) * 4 + col
                base = base + jnp.where(end == k, at, 0)
            score = parts[0, batch, i * count:(i + 1) * count, :]
            for other in range(1, layers):
                score = score + parts[other, batch, i * count:(i + 1) * count, :]
            out_ref[pl.ds(pl.multiple_of(base * count, count), count), :] = score

    for step, (batch, piece) in enumerate(steps):
        communicate(step)
        if step == 0:
            load_acts.wait()
            load_grads.wait()
        multiply(batch, piece)
        if piece == 0 and batch > 0:
            finish(batch - 1)
        if piece == len(widths) - 1:
            for k in range(1, layers):
                share(batch, k, layer).start()
    communicate(len(steps))
    finish(steps[-1][0])

    for k in range(half):
        def sent(k=k):
            for what, *args in sum(events[k], []):
                if what == "send":
                    send(*args).wait_send()

        pl.when(end == k)(sent)
    for batch in range(steps[-1][0] + 1):
        for k in range(1, layers):
            share(batch, k, layer).wait_send()


def shards(nz, layers, layer_inputs, output_grads, input_factors, output_factors):
    count, _, rank, d_in = input_factors.shape
    d_out = output_factors.shape[3]
    tokens = layer_inputs.shape[1]
    rows, cut = count * rank, d_in // CUTS
    widths = (cut,) * CUTS + (d_out,)
    slots = 4 * nz
    queue = max(len(items) for items in simulate(nz, widths)[0].values())
    dma = pltpu.SemaphoreType.DMA
    return pl.pallas_call(
        functools.partial(kernel, nz, layers, count, rank, widths),
        out_shape=jax.ShapeDtypeStruct((slots * count, tokens), jnp.float32),
        in_specs=[pl.BlockSpec(memory_space=pl.ANY)] * 4,
        out_specs=pl.BlockSpec(memory_space=pltpu.VMEM),
        scratch_shapes=[
            pltpu.VMEM((count, rank, d_in), jnp.bfloat16),
            pltpu.VMEM((count, rank, d_out), jnp.bfloat16),
            pltpu.VMEM((CUTS, slots * rows, cut), jnp.bfloat16),
            pltpu.VMEM((slots * rows, d_out), jnp.bfloat16),
            pltpu.VMEM((tokens, d_in), jnp.bfloat16),
            pltpu.VMEM((tokens, d_out), jnp.bfloat16),
            pltpu.VMEM((BATCH * rows, tokens), jnp.float32),
            pltpu.VMEM((layers, slots // BATCH, BATCH * count, tokens), jnp.float32),
            dma((4,)),
            dma((slots, CUTS + 1)),
            dma((4, queue)),
            dma((slots // BATCH, layers)),
            dma((slots // BATCH, layers)),
        ],
        compiler_params=pltpu.CompilerParams(
            collective_id=0, has_side_effects=True, vmem_limit_bytes=60 * 1024 * 1024
        ),
    )(input_factors[:, 0], output_factors[:, 0], layer_inputs[0], output_grads[0])


def solution(mesh):
    in_specs = (
        P("layer", "dp", None),
        P("layer", "dp", None),
        P("dp", "layer", None, None),
        P("dp", "layer", None, None),
    )
    body = functools.partial(shards, mesh.shape["dp"] // 4, mesh.shape["layer"])
    return jax.shard_map(body, mesh=mesh, in_specs=in_specs, out_specs=P(None, "dp"), check_vma=False)
```

```python
import functools

import jax
import jax.numpy as jnp
from jax import lax
from jax.experimental import pallas as pl
from jax.experimental.pallas import tpu as pltpu
from jax.sharding import PartitionSpec as P

MESH = pl.DeviceIdType.MESH
OWN, ACROSS_X, ACROSS_Y, DIAG = range(4)
LINKS = ("x", "y", "in", "ex")
CUTS = 2
LIMIT = 48
BATCH = 4
AHEAD = 2
LATENCY = 1.6
RATE = 730.0
COMPUTE = 0.5
TURN = 0.9
BEGIN = 2.5
TUNED = {
    4: {
        (0, "x"): ((ACROSS_Y, 0), (OWN, 2), (OWN, 0), (ACROSS_Y, 2), (OWN, 1), (OWN, 3)),
        (0, "in"): ((OWN, 0), (DIAG, 2), (DIAG, 0)),
        (1, "x"): ((ACROSS_Y, 1), (OWN, 3), (OWN, 1), (OWN, 0), (ACROSS_Y, 3), (OWN, 2)),
        (1, "in"): ((OWN, 1), (OWN, 0)),
        (1, "ex"): ((OWN, 2), (OWN, 3), (DIAG, 1), (OWN, 1), (DIAG, 3)),
    }
}


def rank_of(nz, end, link, kind, level, piece):
    if link == "y":
        link, kind = "x", {ACROSS_X: ACROSS_Y}.get(kind, kind)
    if nz in TUNED:
        return TUNED[nz][end, link].index((kind, level)), piece
    away = abs(level - end)
    if link == "x":
        return away + (0.5 if kind != OWN else 0.0), piece
    return away + (1.5 if kind != OWN else 0.0), piece


def receiver(half, nz, end, link, level):
    if link in ("x", "y"):
        return end, level
    if link == "ex":
        return end - 1, level
    return (end + 1, level) if end + 1 < half else (end, nz - 1 - level)


def simulate(nz, widths):
    half, pieces = nz // 2, range(len(widths))
    todo, avail = {}, {}
    for end in range(half):
        queue = {link: [] for link in LINKS}
        for level in range(nz):
            for piece in pieces:
                queue["x"].append((OWN, level, piece, ACROSS_X))
                queue["y"].append((OWN, level, piece, ACROSS_Y))
                if level % 2 == end % 2:
                    if (level // 2 + piece) % 2 == 0:
                        queue["x"].append((ACROSS_Y, level, piece, DIAG))
                    else:
                        queue["y"].append((ACROSS_X, level, piece, DIAG))
                    queue["in" if end % 2 == 0 else "ex"].append((DIAG, level, piece, DIAG))
                if level <= end:
                    queue["in"].append((OWN, level, piece, OWN))
                if level >= end > 0:
                    queue["ex"].append((OWN, level, piece, OWN))
        for piece in pieces:
            avail[end, OWN, end, piece] = 0.0
        todo.update({(end, link): items for link, items in queue.items() if items})
    free = {key: 0.0 for key in todo}
    sent = {key: [] for key in todo}
    while any(todo.values()):
        best = None
        for key, items in todo.items():
            for item in items:
                start = max(free[key], avail.get((key[0], *item[:3]), 1e9))
                if best is None or start < best[0] - 1e-9:
                    best = (start, key, [])
                if best[1] == key and start <= best[0] + 1e-9:
                    best[2].append(item)
        start, (end, link), ready = best
        item = min(ready, key=lambda it: rank_of(nz, end, link, *it[:3]))
        todo[end, link].remove(item)
        free[end, link] = start + widths[item[2]] / RATE
        there, level = receiver(half, nz, end, link, item[1])
        avail[there, item[3], level, item[2]] = free[end, link] + LATENCY
        sent[end, link].append((start, item))
    return sent, avail


def plan(nz, widths):
    half, pieces = nz // 2, len(widths)
    sent, avail = simulate(nz, widths)
    slot = {}
    for end in range(half):
        shares = [(kind, level) for kind in range(4) for level in range(nz)]
        shares.sort(key=lambda s: (s != (OWN, end), max(avail[end, *s, p] for p in range(pieces))))
        slot[end] = {share: at for at, share in enumerate(shares)}
    steps = [(None, piece) for piece in range(pieces)]
    steps += [(batch, piece) for batch in range(4 * nz // BATCH) for piece in range(pieces)]
    events = {}
    for end in range(half):
        found = []
        for (sender, link), items in sent.items():
            if sender != end:
                continue
            at = 0.0
            for i, (start, (kind, level, piece, arrives)) in enumerate(items):
                at = max(at, avail[end, kind, level, piece], items[i - AHEAD][0] if i >= AHEAD else 0.0)
                there, counted = receiver(half, nz, end, link, level)
                found.append((at, 0, len(found), ("send", link, i, slot[end][kind, level], slot[there][arrives, counted], piece)))
        order = sorted(found)
        events[end], clock, done = [], BEGIN, 0
        members = {}
        for share, at in slot[end].items():
            members.setdefault(at // BATCH, []).append((share, at))
        for batch, piece in steps:
            need = [(avail[end, *share, piece], at) for share, at in members.get(batch, [])]
            clock = max([clock] + [t for t, _ in need])
            part = []
            while done < len(order) and order[done][0] <= clock:
                part.append(order[done])
                done += 1
            part += [(t, 1, at, ("wait", at, piece)) for t, at in need]
            events[end].append([event for *_, event in sorted(part)])
            clock += (TURN if batch is None else COMPUTE) * widths[piece] / 1024
        events[end].append([event for *_, event in order[done:]])
    return slot, steps, events


def kernel(nz, layers, count, rank, widths, in_hbm, ofac_hbm, acts_hbm, grads_hbm, out_ref,
           raw_in, raw_out, slots_in, slots_out, acts, grads, acts_t, grads_t, total, parts,
           load_sem, recv_sem, send_sem, psend_sem, precv_sem):
    me = lax.axis_index("dp")
    layer = lax.axis_index("layer")
    x, y, z = me % 2, (me // 2) % 2, me // 4
    half = nz // 2
    rows = count * rank
    tokens = acts.shape[0]
    cut = slots_in.shape[2]
    low = z < half
    end = jnp.where(low, z, nz - 1 - z)
    inward = jnp.where(low, 4, 4 * nz - 4)
    target = {
        "x": {"dp": me + 1 - 2 * x},
        "y": {"dp": me + 2 - 4 * y},
        "in": {"dp": (me + inward) % (4 * nz)},
        "ex": {"dp": (me + 4 * nz - inward) % (4 * nz)},
    }
    slot, steps, events = plan(nz, widths)

    load_in = pltpu.make_async_copy(in_hbm, raw_in, load_sem.at[0])
    load_out = pltpu.make_async_copy(ofac_hbm, raw_out, load_sem.at[1])
    load_in.start()
    load_out.start()

    def load(piece):
        if piece == len(widths) - 1:
            return pltpu.make_async_copy(grads_hbm, grads, load_sem.at[2 + piece])
        span = pl.ds(piece * cut, cut)
        return pltpu.make_async_copy(acts_hbm.at[:, span], acts.at[:, span], load_sem.at[2 + piece])

    for piece in range(len(widths)):
        load(piece).start()

    barrier = pltpu.get_barrier_semaphore()
    for link in ("x", "y", "in"):
        pl.semaphore_signal(barrier, inc=1, device_id=target[link], device_id_type=MESH)
    for k in range(1, layers):
        pl.semaphore_signal(barrier, inc=1, device_id={"layer": (layer + k) % layers}, device_id_type=MESH)

    @pl.when(end > 0)
    def _():
        pl.semaphore_signal(barrier, inc=1, device_id=target["ex"], device_id_type=MESH)

    load_in.wait()
    load_out.wait()
    for piece in range(len(widths) - 1):
        own = jnp.swapaxes(raw_in[:, :, piece * cut:(piece + 1) * cut], 0, 1).reshape(rows, cut)
        slots_in[piece, :rows, :] = own
    slots_out[:rows, :] = jnp.swapaxes(raw_out[...], 0, 1).reshape(rows, slots_out.shape[1])
    pl.semaphore_wait(barrier, 3 + layers - 1 + jnp.where(end > 0, 1, 0))

    def held(at, piece):
        span = pl.ds(at * rows, rows)
        return slots_in.at[piece, span, :] if piece < len(widths) - 1 else slots_out.at[span, :]

    def send(link, i, source, dest, piece):
        return pltpu.make_async_remote_copy(
            src_ref=held(source, piece),
            dst_ref=held(dest, piece),
            send_sem=send_sem.at[LINKS.index(link), i],
            recv_sem=recv_sem.at[dest, piece],
            device_id=target[link],
            device_id_type=MESH,
        )

    def arrived(at, piece):
        pltpu.make_async_remote_copy(
            src_ref=held(at, piece),
            dst_ref=held(at, piece),
            send_sem=send_sem.at[0, 0],
            recv_sem=recv_sem.at[at, piece],
            device_id=target["x"],
            device_id_type=MESH,
        ).wait_recv()

    seen = {k: {(0, piece) for piece in range(len(widths))} for k in range(half)}

    def communicate(step):
        for k in range(half):
            def act(k=k):
                for what, *args in events[k][step]:
                    source, piece = (args[2], args[4]) if what == "send" else args
                    if (source, piece) not in seen[k]:
                        seen[k].add((source, piece))
                        arrived(source, piece)
                    if what == "send":
                        send(*args).start()

            if events[k][step]:
                pl.when(end == k)(act)

    group = BATCH * rows
    def turn(piece):
        load(piece).wait()
        if piece == len(widths) - 1:
            grads_t[...] = grads[...].T
        else:
            acts_t[piece * cut:(piece + 1) * cut, :] = acts[:, piece * cut:(piece + 1) * cut].T

    def multiply(batch, piece):
        span = slice(batch * group, (batch + 1) * group)
        if piece < len(widths) - 1:
            right = acts_t[piece * cut:(piece + 1) * cut, :]
            term = jnp.dot(slots_in[piece, span, :], right, preferred_element_type=jnp.float32)
            total[...] = term if piece == 0 else total[...] + term
        else:
            proj_out = jnp.dot(slots_out[span, :], grads_t[...], preferred_element_type=jnp.float32)
            joined = (total[...] * proj_out).reshape(BATCH, rank, count, tokens)
            parts[layer, batch] = jnp.sum(joined, axis=1).reshape(BATCH * count, tokens)

    def share(batch, k, to):
        return pltpu.make_async_remote_copy(
            src_ref=parts.at[to, batch],
            dst_ref=parts.at[to, batch],
            send_sem=psend_sem.at[batch, k],
            recv_sem=precv_sem.at[batch, to],
            device_id={"layer": (layer + k) % layers},
            device_id_type=MESH,
        )

    def finish(batch):
        for k in range(1, layers):
            share(batch, k, (layer + k) % layers).wait_recv()
        for i in range(BATCH):
            base = 0
            for k in range(half):
                kind, level = [share for share, at in slot[k].items() if at == batch * BATCH + i][0]
                col = ((1 - y) if kind in (ACROSS_Y, DIAG) else y) * 2 + ((1 - x) if kind in (ACROSS_X, DIAG) else x)
                at = jnp.where(low, level, nz - 1 - level) * 4 + col
                base = base + jnp.where(end == k, at, 0)
            score = parts[0, batch, i * count:(i + 1) * count, :]
            for other in range(1, layers):
                score = score + parts[other, batch, i * count:(i + 1) * count, :]
            out_ref[pl.ds(pl.multiple_of(base * count, count), count), :] = score

    for step, (batch, piece) in enumerate(steps):
        communicate(step)
        if batch is None:
            turn(piece)
            continue
        multiply(batch, piece)
        if piece == 0 and batch > 0:
            finish(batch - 1)
        if piece == len(widths) - 1:
            for k in range(1, layers):
                share(batch, k, layer).start()
    communicate(len(steps))
    finish(steps[-1][0])

    for k in range(half):
        def sent(k=k):
            for what, *args in sum(events[k], []):
                if what == "send":
                    send(*args).wait_send()

        pl.when(end == k)(sent)
    for batch in range(steps[-1][0] + 1):
        for k in range(1, layers):
            share(batch, k, layer).wait_send()


def shards(nz, layers, layer_inputs, output_grads, input_factors, output_factors):
    count, _, rank, d_in = input_factors.shape
    d_out = output_factors.shape[3]
    tokens = layer_inputs.shape[1]
    rows, cut = count * rank, d_in // CUTS
    widths = (cut,) * CUTS + (d_out,)
    slots = 4 * nz
    queue = max(len(items) for items in simulate(nz, widths)[0].values())
    dma = pltpu.SemaphoreType.DMA
    return pl.pallas_call(
        functools.partial(kernel, nz, layers, count, rank, widths),
        out_shape=jax.ShapeDtypeStruct((slots * count, tokens), jnp.float32),
        in_specs=[pl.BlockSpec(memory_space=pltpu.HBM)] * 4,
        out_specs=pl.BlockSpec(memory_space=pltpu.VMEM),
        scratch_shapes=[
            pltpu.VMEM((count, rank, d_in), jnp.bfloat16),
            pltpu.VMEM((count, rank, d_out), jnp.bfloat16),
            pltpu.VMEM((CUTS, slots * rows, cut), jnp.bfloat16),
            pltpu.VMEM((slots * rows, d_out), jnp.bfloat16),
            pltpu.VMEM((tokens, d_in), jnp.bfloat16),
            pltpu.VMEM((tokens, d_out), jnp.bfloat16),
            pltpu.VMEM((d_in, tokens), jnp.bfloat16),
            pltpu.VMEM((d_out, tokens), jnp.bfloat16),
            pltpu.VMEM((BATCH * rows, tokens), jnp.float32),
            pltpu.VMEM((layers, slots // BATCH, BATCH * count, tokens), jnp.float32),
            dma((CUTS + 3,)),
            dma((slots, CUTS + 1)),
            dma((4, queue)),
            dma((slots // BATCH, layers)),
            dma((slots // BATCH, layers)),
        ],
        compiler_params=pltpu.CompilerParams(
            collective_id=0, has_side_effects=True, vmem_limit_bytes=LIMIT * 1024 * 1024
        ),
    )(*[pltpu.with_memory_space_constraint(a, pltpu.HBM) for a in (input_factors[:, 0], output_factors[:, 0], layer_inputs[0], output_grads[0])])


def solution(mesh):
    in_specs = (
        P("layer", "dp", None),
        P("layer", "dp", None),
        P("dp", "layer", None, None),
        P("dp", "layer", None, None),
    )
    body = functools.partial(shards, mesh.shape["dp"] // 4, mesh.shape["layer"])
    return jax.shard_map(body, mesh=mesh, in_specs=in_specs, out_specs=P(None, "dp"), check_vma=False)
```

```python
import functools

import jax
import jax.numpy as jnp
from jax import lax
from jax.experimental import pallas as pl
from jax.experimental.pallas import tpu as pltpu
from jax.sharding import PartitionSpec as P

MESH = pl.DeviceIdType.MESH
OWN, ACROSS_X, ACROSS_Y, DIAG = range(4)
LINKS = ("x", "y", "in", "ex")
CUTS = 2
LIMIT = 48
BATCH = 4
AHEAD = 2
LATENCY = 1.6
RATE = 730.0
COMPUTE = 0.5
TURN = 0.9
BEGIN = 2.5
TUNED = {
    4: {
        (0, "x"): ((OWN, 2), (ACROSS_Y, 2), (ACROSS_Y, 0), (OWN, 0), (OWN, 1), (OWN, 3)),
        (0, "in"): ((OWN, 0), (DIAG, 2), (DIAG, 0)),
        (1, "x"): ((OWN, 3), (OWN, 1), (ACROSS_Y, 3), (ACROSS_Y, 1), (OWN, 2), (OWN, 0)),
        (1, "in"): ((OWN, 1), (OWN, 0)),
        (1, "ex"): ((OWN, 1), (OWN, 2), (DIAG, 1), (OWN, 3), (DIAG, 3)),
    }
}


def rank_of(nz, end, link, kind, level, piece):
    if link == "y":
        link, kind = "x", {ACROSS_X: ACROSS_Y}.get(kind, kind)
    if nz in TUNED:
        return TUNED[nz][end, link].index((kind, level)), piece
    away = abs(level - end)
    if link == "x":
        return away + (0.5 if kind != OWN else 0.0), piece
    return away + (1.5 if kind != OWN else 0.0), piece


def receiver(half, nz, end, link, level):
    if link in ("x", "y"):
        return end, level
    if link == "ex":
        return end - 1, level
    return (end + 1, level) if end + 1 < half else (end, nz - 1 - level)


def simulate(nz, widths):
    half, pieces = nz // 2, range(len(widths))
    todo, avail = {}, {}
    for end in range(half):
        queue = {link: [] for link in LINKS}
        for level in range(nz):
            for piece in pieces:
                queue["x"].append((OWN, level, piece, ACROSS_X))
                queue["y"].append((OWN, level, piece, ACROSS_Y))
                if level % 2 == end % 2:
                    if (level // 2 + piece) % 2 == 0:
                        queue["x"].append((ACROSS_Y, level, piece, DIAG))
                    else:
                        queue["y"].append((ACROSS_X, level, piece, DIAG))
                    queue["in" if end % 2 == 0 else "ex"].append((DIAG, level, piece, DIAG))
                if level <= end:
                    queue["in"].append((OWN, level, piece, OWN))
                if level >= end > 0:
                    queue["ex"].append((OWN, level, piece, OWN))
        for piece in pieces:
            avail[end, OWN, end, piece] = 0.0
        todo.update({(end, link): items for link, items in queue.items() if items})
    free = {key: 0.0 for key in todo}
    sent = {key: [] for key in todo}
    while any(todo.values()):
        best = None
        for key, items in todo.items():
            for item in items:
                start = max(free[key], avail.get((key[0], *item[:3]), 1e9))
                if best is None or start < best[0] - 1e-9:
                    best = (start, key, [])
                if best[1] == key and start <= best[0] + 1e-9:
                    best[2].append(item)
        start, (end, link), ready = best
        item = min(ready, key=lambda it: rank_of(nz, end, link, *it[:3]))
        todo[end, link].remove(item)
        free[end, link] = start + widths[item[2]] / RATE
        there, level = receiver(half, nz, end, link, item[1])
        avail[there, item[3], level, item[2]] = free[end, link] + LATENCY
        sent[end, link].append((start, item))
    return sent, avail


def plan(nz, widths):
    half, pieces = nz // 2, len(widths)
    sent, avail = simulate(nz, widths)
    slot = {}
    for end in range(half):
        shares = [(kind, level) for kind in range(4) for level in range(nz)]
        shares.sort(key=lambda s: (s != (OWN, end), max(avail[end, *s, p] for p in range(pieces))))
        slot[end] = {share: at for at, share in enumerate(shares)}
    steps = [(None, piece) for piece in range(pieces)]
    steps += [(batch, piece) for batch in range(4 * nz // BATCH) for piece in range(pieces)]
    events = {}
    for end in range(half):
        found = []
        for (sender, link), items in sent.items():
            if sender != end:
                continue
            at = 0.0
            for i, (start, (kind, level, piece, arrives)) in enumerate(items):
                at = max(at, avail[end, kind, level, piece], items[i - AHEAD][0] if i >= AHEAD else 0.0)
                there, counted = receiver(half, nz, end, link, level)
                found.append((at, 0, len(found), ("send", link, i, slot[end][kind, level], slot[there][arrives, counted], piece)))
        order = sorted(found)
        events[end], clock, done = [], BEGIN, 0
        members = {}
        for share, at in slot[end].items():
            members.setdefault(at // BATCH, []).append((share, at))
        for batch, piece in steps:
            need = [(avail[end, *share, piece], at) for share, at in members.get(batch, [])]
            clock = max([clock] + [t for t, _ in need])
            part = []
            while done < len(order) and order[done][0] <= clock:
                part.append(order[done])
                done += 1
            part += [(t, 1, at, ("wait", at, piece)) for t, at in need]
            events[end].append([event for *_, event in sorted(part)])
            clock += (TURN if batch is None else COMPUTE) * widths[piece] / 1024
        events[end].append([event for *_, event in order[done:]])
    return slot, steps, events


def kernel(nz, layers, count, rank, widths, in_hbm, ofac_hbm, acts_hbm, grads_hbm, out_ref,
           raw_in, raw_out, slots_in, slots_out, acts, grads, acts_t, grads_t, total, parts,
           load_sem, recv_sem, send_sem, psend_sem, precv_sem):
    me = lax.axis_index("dp")
    layer = lax.axis_index("layer")
    x, y, z = me % 2, (me // 2) % 2, me // 4
    half = nz // 2
    rows = count * rank
    tokens = acts.shape[0]
    cut = slots_in.shape[2]
    low = z < half
    end = jnp.where(low, z, nz - 1 - z)
    inward = jnp.where(low, 4, 4 * nz - 4)
    target = {
        "x": {"dp": me + 1 - 2 * x},
        "y": {"dp": me + 2 - 4 * y},
        "in": {"dp": (me + inward) % (4 * nz)},
        "ex": {"dp": (me + 4 * nz - inward) % (4 * nz)},
    }
    slot, steps, events = plan(nz, widths)

    load_in = pltpu.make_async_copy(in_hbm, raw_in, load_sem.at[0])
    load_out = pltpu.make_async_copy(ofac_hbm, raw_out, load_sem.at[1])
    load_in.start()
    load_out.start()

    def load(piece):
        if piece == len(widths) - 1:
            return pltpu.make_async_copy(grads_hbm, grads, load_sem.at[2 + piece])
        span = pl.ds(piece * cut, cut)
        return pltpu.make_async_copy(acts_hbm.at[:, span], acts.at[:, span], load_sem.at[2 + piece])

    for piece in range(len(widths)):
        load(piece).start()

    barrier = pltpu.get_barrier_semaphore()
    for link in ("x", "y", "in"):
        pl.semaphore_signal(barrier, inc=1, device_id=target[link], device_id_type=MESH)
    for k in range(1, layers):
        pl.semaphore_signal(barrier, inc=1, device_id={"layer": (layer + k) % layers}, device_id_type=MESH)

    @pl.when(end > 0)
    def _():
        pl.semaphore_signal(barrier, inc=1, device_id=target["ex"], device_id_type=MESH)

    load_in.wait()
    load_out.wait()
    for piece in range(len(widths) - 1):
        own = jnp.swapaxes(raw_in[:, :, piece * cut:(piece + 1) * cut], 0, 1).reshape(rows, cut)
        slots_in[piece, :rows, :] = own
    slots_out[:rows, :] = jnp.swapaxes(raw_out[...], 0, 1).reshape(rows, slots_out.shape[1])
    pl.semaphore_wait(barrier, 3 + layers - 1 + jnp.where(end > 0, 1, 0))

    def held(at, piece):
        span = pl.ds(at * rows, rows)
        return slots_in.at[piece, span, :] if piece < len(widths) - 1 else slots_out.at[span, :]

    def send(link, i, source, dest, piece):
        return pltpu.make_async_remote_copy(
            src_ref=held(source, piece),
            dst_ref=held(dest, piece),
            send_sem=send_sem.at[LINKS.index(link), i],
            recv_sem=recv_sem.at[dest, piece],
            device_id=target[link],
            device_id_type=MESH,
        )

    def arrived(at, piece):
        pltpu.make_async_remote_copy(
            src_ref=held(at, piece),
            dst_ref=held(at, piece),
            send_sem=send_sem.at[0, 0],
            recv_sem=recv_sem.at[at, piece],
            device_id=target["x"],
            device_id_type=MESH,
        ).wait_recv()

    seen = {k: {(0, piece) for piece in range(len(widths))} for k in range(half)}

    def communicate(step):
        for k in range(half):
            def act(k=k):
                for what, *args in events[k][step]:
                    source, piece = (args[2], args[4]) if what == "send" else args
                    if (source, piece) not in seen[k]:
                        seen[k].add((source, piece))
                        arrived(source, piece)
                    if what == "send":
                        send(*args).start()

            if events[k][step]:
                pl.when(end == k)(act)

    group = BATCH * rows
    def turn(piece):
        load(piece).wait()
        if piece == len(widths) - 1:
            grads_t[...] = grads[...].T
        else:
            acts_t[piece * cut:(piece + 1) * cut, :] = acts[:, piece * cut:(piece + 1) * cut].T

    def multiply(batch, piece):
        span = slice(batch * group, (batch + 1) * group)
        if piece < len(widths) - 1:
            right = acts_t[piece * cut:(piece + 1) * cut, :]
            term = jnp.dot(slots_in[piece, span, :], right, preferred_element_type=jnp.float32)
            total[...] = term if piece == 0 else total[...] + term
        else:
            proj_out = jnp.dot(slots_out[span, :], grads_t[...], preferred_element_type=jnp.float32)
            joined = (total[...] * proj_out).reshape(BATCH, rank, count, tokens)
            parts[layer, batch] = jnp.sum(joined, axis=1).reshape(BATCH * count, tokens)

    def share(batch, k, to):
        return pltpu.make_async_remote_copy(
            src_ref=parts.at[to, batch],
            dst_ref=parts.at[to, batch],
            send_sem=psend_sem.at[batch, k],
            recv_sem=precv_sem.at[batch, to],
            device_id={"layer": (layer + k) % layers},
            device_id_type=MESH,
        )

    def finish(batch):
        for k in range(1, layers):
            share(batch, k, (layer + k) % layers).wait_recv()
        for i in range(BATCH):
            base = 0
            for k in range(half):
                kind, level = [share for share, at in slot[k].items() if at == batch * BATCH + i][0]
                col = ((1 - y) if kind in (ACROSS_Y, DIAG) else y) * 2 + ((1 - x) if kind in (ACROSS_X, DIAG) else x)
                at = jnp.where(low, level, nz - 1 - level) * 4 + col
                base = base + jnp.where(end == k, at, 0)
            score = parts[0, batch, i * count:(i + 1) * count, :]
            for other in range(1, layers):
                score = score + parts[other, batch, i * count:(i + 1) * count, :]
            out_ref[pl.ds(pl.multiple_of(base * count, count), count), :] = score

    for step, (batch, piece) in enumerate(steps):
        communicate(step)
        if batch is None:
            turn(piece)
            continue
        multiply(batch, piece)
        if piece == 0 and batch > 0:
            finish(batch - 1)
        if piece == len(widths) - 1:
            for k in range(1, layers):
                share(batch, k, layer).start()
    communicate(len(steps))
    finish(steps[-1][0])

    for k in range(half):
        def sent(k=k):
            for what, *args in sum(events[k], []):
                if what == "send":
                    send(*args).wait_send()

        pl.when(end == k)(sent)
    for batch in range(steps[-1][0] + 1):
        for k in range(1, layers):
            share(batch, k, layer).wait_send()


def shards(nz, layers, layer_inputs, output_grads, input_factors, output_factors):
    count, _, rank, d_in = input_factors.shape
    d_out = output_factors.shape[3]
    tokens = layer_inputs.shape[1]
    rows, cut = count * rank, d_in // CUTS
    widths = (cut,) * CUTS + (d_out,)
    slots = 4 * nz
    queue = max(len(items) for items in simulate(nz, widths)[0].values())
    dma = pltpu.SemaphoreType.DMA
    return pl.pallas_call(
        functools.partial(kernel, nz, layers, count, rank, widths),
        out_shape=jax.ShapeDtypeStruct((slots * count, tokens), jnp.float32),
        in_specs=[pl.BlockSpec(memory_space=pltpu.HBM)] * 4,
        out_specs=pl.BlockSpec(memory_space=pltpu.VMEM),
        scratch_shapes=[
            pltpu.VMEM((count, rank, d_in), jnp.bfloat16),
            pltpu.VMEM((count, rank, d_out), jnp.bfloat16),
            pltpu.VMEM((CUTS, slots * rows, cut), jnp.bfloat16),
            pltpu.VMEM((slots * rows, d_out), jnp.bfloat16),
            pltpu.VMEM((tokens, d_in), jnp.bfloat16),
            pltpu.VMEM((tokens, d_out), jnp.bfloat16),
            pltpu.VMEM((d_in, tokens), jnp.bfloat16),
            pltpu.VMEM((d_out, tokens), jnp.bfloat16),
            pltpu.VMEM((BATCH * rows, tokens), jnp.float32),
            pltpu.VMEM((layers, slots // BATCH, BATCH * count, tokens), jnp.float32),
            dma((CUTS + 3,)),
            dma((slots, CUTS + 1)),
            dma((4, queue)),
            dma((slots // BATCH, layers)),
            dma((slots // BATCH, layers)),
        ],
        compiler_params=pltpu.CompilerParams(
            collective_id=0, has_side_effects=True, vmem_limit_bytes=LIMIT * 1024 * 1024
        ),
    )(*[pltpu.with_memory_space_constraint(a, pltpu.HBM) for a in (input_factors[:, 0], output_factors[:, 0], layer_inputs[0], output_grads[0])])


def solution(mesh):
    in_specs = (
        P("layer", "dp", None),
        P("layer", "dp", None),
        P("dp", "layer", None, None),
        P("dp", "layer", None, None),
    )
    body = functools.partial(shards, mesh.shape["dp"] // 4, mesh.shape["layer"])
    return jax.shard_map(body, mesh=mesh, in_specs=in_specs, out_specs=P(None, "dp"), check_vma=False)
```

```python
import functools

import jax
import jax.numpy as jnp
from jax import lax
from jax.experimental import pallas as pl
from jax.experimental.pallas import tpu as pltpu
from jax.sharding import PartitionSpec as P

MESH = pl.DeviceIdType.MESH
OWN, ACROSS_X, ACROSS_Y, DIAG = range(4)
LINKS = ("x", "y", "in", "ex")
CUTS = 2
LIMIT = 48
BATCH = 4
AHEAD = 2
PARTS = 1
LATENCY = 1.6
RATE = 730.0
COMPUTE = 0.5
TURN = 0.9
BEGIN = 2.5
TUNED = {
    4: {
        (0, "x"): ((OWN, 2), (ACROSS_Y, 2), (ACROSS_Y, 0), (OWN, 0), (OWN, 1), (OWN, 3)),
        (0, "in"): ((OWN, 0), (DIAG, 2), (DIAG, 0)),
        (1, "x"): ((OWN, 3), (OWN, 1), (ACROSS_Y, 3), (ACROSS_Y, 1), (OWN, 2), (OWN, 0)),
        (1, "in"): ((OWN, 1), (OWN, 0)),
        (1, "ex"): ((OWN, 1), (OWN, 2), (DIAG, 1), (OWN, 3), (DIAG, 3)),
    }
}


def rank_of(nz, end, link, kind, level, piece):
    if link == "y":
        link, kind = "x", {ACROSS_X: ACROSS_Y}.get(kind, kind)
    if nz in TUNED:
        return TUNED[nz][end, link].index((kind, level)), piece
    away = abs(level - end)
    if link == "x":
        return away + (0.5 if kind != OWN else 0.0), piece
    return away + (1.5 if kind != OWN else 0.0), piece


def receiver(half, nz, end, link, level):
    if link in ("x", "y"):
        return end, level
    if link == "ex":
        return end - 1, level
    return (end + 1, level) if end + 1 < half else (end, nz - 1 - level)


def simulate(nz, widths):
    half, pieces = nz // 2, range(len(widths))
    todo, avail = {}, {}
    for end in range(half):
        queue = {link: [] for link in LINKS}
        for level in range(nz):
            for piece in pieces:
                queue["x"].append((OWN, level, piece, ACROSS_X))
                queue["y"].append((OWN, level, piece, ACROSS_Y))
                if level % 2 == end % 2:
                    if (level // 2 + piece) % 2 == 0:
                        queue["x"].append((ACROSS_Y, level, piece, DIAG))
                    else:
                        queue["y"].append((ACROSS_X, level, piece, DIAG))
                    queue["in" if end % 2 == 0 else "ex"].append((DIAG, level, piece, DIAG))
                if level <= end:
                    queue["in"].append((OWN, level, piece, OWN))
                if level >= end > 0:
                    queue["ex"].append((OWN, level, piece, OWN))
        for piece in pieces:
            avail[end, OWN, end, piece] = 0.0
        todo.update({(end, link): items for link, items in queue.items() if items})
    free = {key: 0.0 for key in todo}
    sent = {key: [] for key in todo}
    while any(todo.values()):
        best = None
        for key, items in todo.items():
            for item in items:
                start = max(free[key], avail.get((key[0], *item[:3]), 1e9))
                if best is None or start < best[0] - 1e-9:
                    best = (start, key, [])
                if best[1] == key and start <= best[0] + 1e-9:
                    best[2].append(item)
        start, (end, link), ready = best
        item = min(ready, key=lambda it: rank_of(nz, end, link, *it[:3]))
        todo[end, link].remove(item)
        free[end, link] = start + widths[item[2]] / RATE
        there, level = receiver(half, nz, end, link, item[1])
        avail[there, item[3], level, item[2]] = free[end, link] + LATENCY
        sent[end, link].append((start, item))
    return sent, avail


def plan(nz, widths):
    half, pieces = nz // 2, len(widths)
    sent, avail = simulate(nz, widths)
    slot = {}
    for end in range(half):
        shares = [(kind, level) for kind in range(4) for level in range(nz)]
        shares.sort(key=lambda s: (s != (OWN, end), max(avail[end, *s, p] for p in range(pieces))))
        slot[end] = {share: at for at, share in enumerate(shares)}
    steps = [(None, piece) for piece in range(pieces)]
    steps += [(batch, piece) for batch in range(4 * nz // BATCH) for piece in range(pieces)]
    events = {}
    for end in range(half):
        found = []
        for (sender, link), items in sent.items():
            if sender != end:
                continue
            at = 0.0
            for i, (start, (kind, level, piece, arrives)) in enumerate(items):
                at = max(at, avail[end, kind, level, piece], items[i - AHEAD][0] if i >= AHEAD else 0.0)
                there, counted = receiver(half, nz, end, link, level)
                found.append((at, 0, len(found), ("send", link, i, slot[end][kind, level], slot[there][arrives, counted], piece)))
        order = sorted(found)
        events[end], clock, done = [], BEGIN, 0
        members = {}
        for share, at in slot[end].items():
            members.setdefault(at // BATCH, []).append((share, at))
        for batch, piece in steps:
            need = [(avail[end, *share, piece], at) for share, at in members.get(batch, [])]
            clock = max([clock] + [t for t, _ in need])
            part = []
            while done < len(order) and order[done][0] <= clock:
                part.append(order[done])
                done += 1
            part += [(t, 1, at, ("wait", at, piece)) for t, at in need]
            events[end].append([event for *_, event in sorted(part)])
            clock += (TURN if batch is None else COMPUTE) * widths[piece] / 1024
        events[end].append([event for *_, event in order[done:]])
    return slot, steps, events


def kernel(nz, layers, count, rank, widths, in_hbm, ofac_hbm, acts_hbm, grads_hbm, out_ref,
           raw_in, raw_out, slots_in, slots_out, acts, grads, acts_t, grads_t, total, parts,
           load_sem, recv_sem, send_sem, psend_sem, precv_sem):
    me = lax.axis_index("dp")
    layer = lax.axis_index("layer")
    x, y, z = me % 2, (me // 2) % 2, me // 4
    half = nz // 2
    rows = count * rank
    tokens = acts.shape[0]
    cut = slots_in.shape[2]
    low = z < half
    end = jnp.where(low, z, nz - 1 - z)
    inward = jnp.where(low, 4, 4 * nz - 4)
    target = {
        "x": {"dp": me + 1 - 2 * x},
        "y": {"dp": me + 2 - 4 * y},
        "in": {"dp": (me + inward) % (4 * nz)},
        "ex": {"dp": (me + 4 * nz - inward) % (4 * nz)},
    }
    slot, steps, events = plan(nz, widths)

    load_in = pltpu.make_async_copy(in_hbm, raw_in, load_sem.at[0])
    load_out = pltpu.make_async_copy(ofac_hbm, raw_out, load_sem.at[1])
    load_in.start()
    load_out.start()

    def load(piece):
        if piece == len(widths) - 1:
            return pltpu.make_async_copy(grads_hbm, grads, load_sem.at[2 + piece])
        span = pl.ds(piece * cut, cut)
        return pltpu.make_async_copy(acts_hbm.at[:, span], acts.at[:, span], load_sem.at[2 + piece])


    barrier = pltpu.get_barrier_semaphore()
    for link in ("x", "y", "in"):
        pl.semaphore_signal(barrier, inc=1, device_id=target[link], device_id_type=MESH)
    for k in range(1, layers):
        pl.semaphore_signal(barrier, inc=1, device_id={"layer": (layer + k) % layers}, device_id_type=MESH)

    @pl.when(end > 0)
    def _():
        pl.semaphore_signal(barrier, inc=1, device_id=target["ex"], device_id_type=MESH)

    for piece in range(len(widths)):
        load(piece).start()
    load_in.wait()
    load_out.wait()
    for piece in range(len(widths) - 1):
        own = jnp.swapaxes(raw_in[:, :, piece * cut:(piece + 1) * cut], 0, 1).reshape(rows, cut)
        slots_in[piece, :rows, :] = own
    slots_out[:rows, :] = jnp.swapaxes(raw_out[...], 0, 1).reshape(rows, slots_out.shape[1])
    pl.semaphore_wait(barrier, 3 + layers - 1 + jnp.where(end > 0, 1, 0))

    def held(at, piece):
        span = pl.ds(at * rows, rows)
        return slots_in.at[piece, span, :] if piece < len(widths) - 1 else slots_out.at[span, :]

    def send(link, i, source, dest, piece):
        return pltpu.make_async_remote_copy(
            src_ref=held(source, piece),
            dst_ref=held(dest, piece),
            send_sem=send_sem.at[LINKS.index(link), i],
            recv_sem=recv_sem.at[dest, piece],
            device_id=target[link],
            device_id_type=MESH,
        )

    def arrived(at, piece):
        pltpu.make_async_remote_copy(
            src_ref=held(at, piece),
            dst_ref=held(at, piece),
            send_sem=send_sem.at[0, 0],
            recv_sem=recv_sem.at[at, piece],
            device_id=target["x"],
            device_id_type=MESH,
        ).wait_recv()

    seen = {k: {(0, piece) for piece in range(len(widths))} for k in range(half)}

    def communicate(step):
        for k in range(half):
            def act(k=k):
                for what, *args in events[k][step]:
                    source, piece = (args[2], args[4]) if what == "send" else args
                    if (source, piece) not in seen[k]:
                        seen[k].add((source, piece))
                        arrived(source, piece)
                    if what == "send":
                        send(*args).start()

            if events[k][step]:
                pl.when(end == k)(act)

    group = BATCH * rows
    def turn(piece):
        load(piece).wait()
        if piece == len(widths) - 1:
            grads_t[...] = grads[...].T
        else:
            acts_t[piece * cut:(piece + 1) * cut, :] = acts[:, piece * cut:(piece + 1) * cut].T

    def multiply(batch, piece):
        span = slice(batch * group, (batch + 1) * group)
        if piece < len(widths) - 1:
            right = acts_t[piece * cut:(piece + 1) * cut, :]
            term = jnp.dot(slots_in[piece, span, :], right, preferred_element_type=jnp.float32)
            total[...] = term if piece == 0 else total[...] + term
        else:
            proj_out = jnp.dot(slots_out[span, :], grads_t[...], preferred_element_type=jnp.float32)
            joined = (total[...] * proj_out).reshape(BATCH, rank, count, tokens)
            parts[layer, batch] = jnp.sum(joined, axis=1).reshape(BATCH * count, tokens)

    def share(batch, k, to):
        return pltpu.make_async_remote_copy(
            src_ref=parts.at[to, batch],
            dst_ref=parts.at[to, batch],
            send_sem=psend_sem.at[batch, k],
            recv_sem=precv_sem.at[batch, to],
            device_id={"layer": (layer + k) % layers},
            device_id_type=MESH,
        )

    def finish(batch):
        for k in range(1, layers):
            share(batch, k, (layer + k) % layers).wait_recv()
        for i in range(BATCH):
            base = 0
            for k in range(half):
                kind, level = [share for share, at in slot[k].items() if at == batch * BATCH + i][0]
                col = ((1 - y) if kind in (ACROSS_Y, DIAG) else y) * 2 + ((1 - x) if kind in (ACROSS_X, DIAG) else x)
                at = jnp.where(low, level, nz - 1 - level) * 4 + col
                base = base + jnp.where(end == k, at, 0)
            score = parts[0, batch, i * count:(i + 1) * count, :]
            for other in range(1, layers):
                score = score + parts[other, batch, i * count:(i + 1) * count, :]
            out_ref[pl.ds(pl.multiple_of(base * count, count), count), :] = score

    for step, (batch, piece) in enumerate(steps):
        communicate(step)
        if batch is None:
            turn(piece)
            continue
        multiply(batch, piece)
        if piece == 0 and batch > 0:
            finish(batch - 1)
        if piece == len(widths) - 1:
            for k in range(1, layers):
                share(batch, k, layer).start()
    communicate(len(steps))
    finish(steps[-1][0])

    for k in range(half):
        def sent(k=k):
            for what, *args in sum(events[k], []):
                if what == "send":
                    send(*args).wait_send()

        pl.when(end == k)(sent)
    for batch in range(steps[-1][0] + 1):
        for k in range(1, layers):
            share(batch, k, layer).wait_send()


def store(scores_ref, out_ref, sem):
    rows = scores_ref.shape[0] // PARTS
    copies = []
    for part in range(PARTS):
        span = pl.ds(part * rows, rows)
        copies.append(pltpu.make_async_copy(scores_ref.at[span, :], out_ref.at[span, :], sem.at[part]))
        copies[-1].start()
    for copy in copies:
        copy.wait()


def shards(nz, layers, layer_inputs, output_grads, input_factors, output_factors):
    count, _, rank, d_in = input_factors.shape
    d_out = output_factors.shape[3]
    tokens = layer_inputs.shape[1]
    rows, cut = count * rank, d_in // CUTS
    widths = (cut,) * CUTS + (d_out,)
    slots = 4 * nz
    queue = max(len(items) for items in simulate(nz, widths)[0].values())
    dma = pltpu.SemaphoreType.DMA
    scores = pl.pallas_call(
        functools.partial(kernel, nz, layers, count, rank, widths),
        out_shape=jax.ShapeDtypeStruct((slots * count, tokens), jnp.float32),
        in_specs=[pl.BlockSpec(memory_space=pltpu.HBM)] * 4,
        out_specs=pl.BlockSpec(memory_space=pltpu.VMEM),
        scratch_shapes=[
            pltpu.VMEM((count, rank, d_in), jnp.bfloat16),
            pltpu.VMEM((count, rank, d_out), jnp.bfloat16),
            pltpu.VMEM((CUTS, slots * rows, cut), jnp.bfloat16),
            pltpu.VMEM((slots * rows, d_out), jnp.bfloat16),
            pltpu.VMEM((tokens, d_in), jnp.bfloat16),
            pltpu.VMEM((tokens, d_out), jnp.bfloat16),
            pltpu.VMEM((d_in, tokens), jnp.bfloat16),
            pltpu.VMEM((d_out, tokens), jnp.bfloat16),
            pltpu.VMEM((BATCH * rows, tokens), jnp.float32),
            pltpu.VMEM((layers, slots // BATCH, BATCH * count, tokens), jnp.float32),
            dma((CUTS + 3,)),
            dma((slots, CUTS + 1)),
            dma((4, queue)),
            dma((slots // BATCH, layers)),
            dma((slots // BATCH, layers)),
        ],
        compiler_params=pltpu.CompilerParams(
            collective_id=0, has_side_effects=True, vmem_limit_bytes=LIMIT * 1024 * 1024
        ),
    )(*[pltpu.with_memory_space_constraint(a, pltpu.HBM) for a in (input_factors[:, 0], output_factors[:, 0], layer_inputs[0], output_grads[0])])
    return pl.pallas_call(
        store,
        out_shape=jax.ShapeDtypeStruct(scores.shape, scores.dtype),
        in_specs=[pl.BlockSpec(memory_space=pltpu.VMEM)],
        out_specs=pl.BlockSpec(memory_space=pltpu.HBM),
        scratch_shapes=[dma((PARTS,))],
        compiler_params=pltpu.CompilerParams(vmem_limit_bytes=8 * 1024 * 1024),
    )(scores)


def solution(mesh):
    in_specs = (
        P("layer", "dp", None),
        P("layer", "dp", None),
        P("dp", "layer", None, None),
        P("dp", "layer", None, None),
    )
    body = functools.partial(shards, mesh.shape["dp"] // 4, mesh.shape["layer"])
    return jax.shard_map(body, mesh=mesh, in_specs=in_specs, out_specs=P(None, "dp"), check_vma=False)
```
